8 devices in a mesh: dp: 8 (over z, y, x, core).
Axes of the slice: x: 2, y: 2, z: 1, core: 2. Of those that a mesh axis runs over, the one named last changes fastest.
Arguments:
- x_embed: bfloat16 [2048, 1024], P('dp')
- positions: int32 [2048], P('dp')
- k_cache: bfloat16 [2, 2048, 32, 16, 64], P(None, 'dp')
- v_cache: bfloat16 [2, 2048, 32, 16, 64], P(None, 'dp')
- ln1_gain: bfloat16 [2, 1024], P(None, 'dp')
- ln1_bias: bfloat16 [2, 1024], P(None, 'dp')
- ln2_gain: bfloat16 [2, 1024], P(None, 'dp')
- ln2_bias: bfloat16 [2, 1024], P(None, 'dp')
- w_qkv: bfloat16 [2, 1024, 3072], P(None, 'dp')
- b_qkv: bfloat16 [2, 3072], P(None, 'dp')
- w_out: bfloat16 [2, 1024, 1024], P(None, 'dp')
- b_out: bfloat16 [2, 1024], P(None, 'dp')
- w_in: bfloat16 [2, 1024, 4096], P(None, 'dp')
- b_in: bfloat16 [2, 4096], P(None, 'dp')
- w_down: bfloat16 [2, 4096, 1024], P(None, 'dp')
- b_down: bfloat16 [2, 1024], P(None, 'dp')
- lnf_gain: bfloat16 [1024], P('dp')
- lnf_bias: bfloat16 [1024], P('dp')
Outputs:
- output 1: bfloat16 [2048, 1024], P('dp')
- output 2: bfloat16 [2, 2048, 32, 16, 64], P(None, 'dp')
- output 3: bfloat16 [2, 2048, 32, 16, 64], P(None, 'dp')
All inputs are finite; a program needn't handle non-finite values.
Results may differ from the reference program's by a relative error of at most 0.00517104.
Values are sent between devices in bfloat16 or wider.
A program may use at most 1 GiB of HBM per device.

```python
import jax
import jax.numpy as jnp
from jax import lax

LAYERS = 2
BATCH = 2048
SMAX = 32
D = 1024
HEADS = 16
FF = 4096
HEAD = 64
ROT = 16

LN_EPS = 1e-5
ROPE_BASE = 10000.0


def setup_inputs(seed: int = 0) -> dict:
    root_key = jax.random.key(seed)
    subkeys = jax.random.split(root_key, 20)

    def normal(key_idx, arr_shape, std_dev):
        return jax.random.normal(subkeys[key_idx], arr_shape, jnp.float32) * std_dev

    cache_shape = (LAYERS, BATCH, SMAX, HEADS, HEAD)
    positions = jax.random.randint(subkeys[1], (BATCH,), 0, SMAX, dtype=jnp.int32)
    positions = positions.at[0].set(SMAX - 1)
    v_mean = normal(3, (LAYERS, BATCH, 1, HEADS, HEAD), 1.0)
    return {
        'x_embed': normal(0, (BATCH, D), 1.0).astype(jnp.bfloat16),
        'positions': positions,
        'k_cache': normal(2, cache_shape, 1.0).astype(jnp.bfloat16),
        'v_cache': (v_mean + normal(4, cache_shape, 0.5)).astype(jnp.bfloat16),
        'ln1_gain': (1.0 + normal(5, (LAYERS, D), 0.2)).astype(jnp.bfloat16),
        'ln1_bias': normal(6, (LAYERS, D), 0.2).astype(jnp.bfloat16),
        'ln2_gain': (1.0 + normal(7, (LAYERS, D), 0.2)).astype(jnp.bfloat16),
        'ln2_bias': normal(8, (LAYERS, D), 0.2).astype(jnp.bfloat16),
        'w_qkv': normal(9, (LAYERS, D, 3 * D), D ** -0.5).astype(jnp.bfloat16),
        'b_qkv': normal(10, (LAYERS, 3 * D), 0.3).astype(jnp.bfloat16),
        'w_out': normal(11, (LAYERS, D, D), D ** -0.5).astype(jnp.bfloat16),
        'b_out': normal(12, (LAYERS, D), 0.3).astype(jnp.bfloat16),
        'w_in': normal(13, (LAYERS, D, FF), D ** -0.5).astype(jnp.bfloat16),
        'b_in': normal(14, (LAYERS, FF), 0.3).astype(jnp.bfloat16),
        'w_down': normal(15, (LAYERS, FF, D), FF ** -0.5).astype(jnp.bfloat16),
        'b_down': normal(16, (LAYERS, D), 0.3).astype(jnp.bfloat16),
        'lnf_gain': (1.0 + normal(17, (D,), 0.2)).astype(jnp.bfloat16),
        'lnf_bias': normal(18, (D,), 0.2).astype(jnp.bfloat16),
    }


def layer_norm(values, ln_gain, ln_bias):
    x_f32 = values.astype(jnp.float32)
    row_mean = jnp.mean(x_f32, axis=-1, keepdims=True)
    centered = x_f32 - row_mean
    row_var = jnp.mean(centered * centered, axis=-1, keepdims=True)
    normed = centered * lax.rsqrt(row_var + LN_EPS)
    return (normed * ln_gain.astype(jnp.float32) + ln_bias.astype(jnp.float32)).astype(jnp.bfloat16)


def rotate(values, cos_t, sin_t):
    half_dim = ROT // 2
    rot_part = values[..., :ROT].astype(jnp.float32)
    turned = jnp.concatenate([-rot_part[..., half_dim:], rot_part[..., :half_dim]], axis=-1)
    mixed = rot_part * cos_t + turned * sin_t
    return jnp.concatenate([mixed.astype(jnp.bfloat16), values[..., ROT:]], axis=-1)


def reference(x_embed, positions, k_cache, v_cache, ln1_gain, ln1_bias, ln2_gain, ln2_bias, w_qkv, b_qkv, w_out, b_out, w_in, b_in, w_down, b_down, lnf_gain, lnf_bias):
    inv_freq = 1.0 / (ROPE_BASE ** (jnp.arange(0, ROT, 2).astype(jnp.float32) / ROT))
    angles = positions.astype(jnp.float32)[:, None] * inv_freq[None, :]
    angles = jnp.concatenate([angles, angles], axis=-1)[:, None, :]
    cos_t = jnp.cos(angles)
    sin_t = jnp.sin(angles)
    slot_ids = jnp.arange(SMAX)
    write_mask = (slot_ids[None, :] == positions[:, None])[:, :, None, None]
    keep_mask = (slot_ids[None, :] <= positions[:, None])[:, None, :]

    def one_layer(hidden, params):
        (k_layer, v_layer, g_one, c_one, g_two, c_two, wqkv_l, bqkv_l, wout_l, bout_l, win_l, bin_l, wdown_l, bdown_l) = params
        h_attn = layer_norm(hidden, g_one, c_one)
        h_mlp = layer_norm(hidden, g_two, c_two)
        qkv_proj = (jnp.dot(h_attn, wqkv_l, preferred_element_type=jnp.float32) + bqkv_l.astype(jnp.float32)).astype(jnp.bfloat16)
        qkv_proj = qkv_proj.reshape(BATCH, HEADS, 3, HEAD)
        q_heads = rotate(qkv_proj[:, :, 0], cos_t, sin_t)
        k_heads = rotate(qkv_proj[:, :, 1], cos_t, sin_t)
        v_heads = qkv_proj[:, :, 2]
        k_layer = jnp.where(write_mask, k_heads[:, None], k_layer)
        v_layer = jnp.where(write_mask, v_heads[:, None], v_layer)
        scores = jnp.einsum('bhd,bshd->bhs', q_heads.astype(jnp.float32), k_layer.astype(jnp.float32)) * (HEAD ** -0.5)
        scores = jnp.where(keep_mask, scores, -jnp.inf)
        attn_probs = jax.nn.softmax(scores, axis=-1).astype(jnp.bfloat16)
        context = jnp.einsum('bhs,bshd->bhd', attn_probs.astype(jnp.float32), v_layer.astype(jnp.float32)).astype(jnp.bfloat16).reshape(BATCH, D)
        attn_out = jnp.dot(context, wout_l, preferred_element_type=jnp.float32) + bout_l.astype(jnp.float32)
        mlp_act = jax.nn.gelu(jnp.dot(h_mlp, win_l, preferred_element_type=jnp.float32) + bin_l.astype(jnp.float32), approximate=False).astype(jnp.bfloat16)
        mlp_out = jnp.dot(mlp_act, wdown_l, preferred_element_type=jnp.float32) + bdown_l.astype(jnp.float32)
        hidden = (hidden.astype(jnp.float32) + attn_out + mlp_out).astype(jnp.bfloat16)
        return hidden, (k_layer, v_layer)

    stacked = (k_cache, v_cache, ln1_gain, ln1_bias, ln2_gain, ln2_bias, w_qkv, b_qkv, w_out, b_out, w_in, b_in, w_down, b_down)
    hidden, (k_new, v_new) = lax.scan(one_layer, x_embed, stacked)
    return layer_norm(hidden, lnf_gain, lnf_bias), k_new, v_new
```

```python
import functools
import jax
import jax.numpy as jnp
from jax import lax
from jax.experimental import pallas as pl
from jax.experimental.pallas import tpu as pltpu
from jax.sharding import PartitionSpec as P

LN_EPS = 1e-5
ROPE_BASE = 10000.0

CORE, XN, YN = 1, 2, 4
D = 1024
BL = 256
SLOTS = 32
HEADS = 16
HEAD = 64
ANY = pl.BlockSpec(memory_space=pl.ANY)
VM = pl.BlockSpec(memory_space=pltpu.VMEM)
SM = pl.BlockSpec(memory_space=pltpu.SMEM)
VMEM_LIMIT = 56 * 2**20


def permute(values, mask):
    return lax.ppermute(values, "dp", [(i, i ^ mask) for i in range(8)])


def cost(flops, nbytes):
    return pl.CostEstimate(flops=flops, bytes_accessed=nbytes, transcendentals=0)


def params(limit=VMEM_LIMIT):
    return pltpu.CompilerParams(vmem_limit_bytes=limit)


def layer_norm_rows(x_bf16, gain, bias):
    x_f32 = x_bf16.astype(jnp.float32)
    row_mean = jnp.mean(x_f32, axis=-1, keepdims=True)
    centered = x_f32 - row_mean
    row_var = jnp.mean(centered * centered, axis=-1, keepdims=True)
    normed = centered * lax.rsqrt(row_var + LN_EPS)
    return (normed * gain + bias).astype(jnp.bfloat16)


def pack_attn_kernel(layer, wqkv, wout, out, sem):
    copies = [
        pltpu.make_async_copy(wqkv.at[layer, :, pl.ds(1024 * b, 1024)], out.at[pl.ds(128 * b, 128)], sem.at[b])
        for b in range(3)
    ]
    copies.append(pltpu.make_async_copy(wout.at[layer], out.at[pl.ds(384, 128)], sem.at[3]))
    for copy in copies:
        copy.start()
    for copy in copies:
        copy.wait()


def pack_attn(layer, wqkv, wout):
    return pl.pallas_call(
        functools.partial(pack_attn_kernel, layer),
        out_shape=jax.ShapeDtypeStruct((512, D), jnp.bfloat16),
        in_specs=[ANY, ANY], out_specs=VM,
        scratch_shapes=[pltpu.SemaphoreType.DMA((4,))],
        compiler_params=params(16 * 2**20),
        cost_estimate=cost(10**6, 2 * 2**20),
        name=f"pack_attn{layer}",
    )(wqkv, wout)


def pack_mlp_kernel(layer, half, win, wdown, mine, other, sem):
    xb = half[0]
    copies = []
    for yy in range(2):
        own_col = pl.multiple_of((2 * yy + xb) * 1024, 1024)
        oth_col = pl.multiple_of((2 * yy + 1 - xb) * 1024, 1024)
        rows = pl.ds(128 * yy, 128)
        copies.append(pltpu.make_async_copy(win.at[layer, :, pl.ds(own_col, 1024)], mine.at[rows], sem.at[yy]))
        copies.append(pltpu.make_async_copy(win.at[layer, :, pl.ds(oth_col, 1024)], other.at[rows], sem.at[2 + yy]))
    copies.append(pltpu.make_async_copy(wdown.at[layer], mine.at[pl.ds(256, 512)], sem.at[4]))
    for copy in copies:
        copy.start()
    for copy in copies:
        copy.wait()


def pack_mlp(layer, half, win, wdown):
    return pl.pallas_call(
        functools.partial(pack_mlp_kernel, layer),
        out_shape=(jax.ShapeDtypeStruct((768, D), jnp.bfloat16), jax.ShapeDtypeStruct((256, D), jnp.bfloat16)),
        in_specs=[SM, ANY, ANY], out_specs=(VM, VM),
        scratch_shapes=[pltpu.SemaphoreType.DMA((5,))],
        compiler_params=params(16 * 2**20),
        cost_estimate=cost(10**6, 4 * 2**20),
        name=f"pack_mlp{layer}",
    )(half, win, wdown)


def spread_attn(own):
    from_x = permute(own, XN)
    from_y = permute(own, YN)
    diag_lo = permute(from_x[:256], YN)
    diag_hi = permute(from_y[256:], XN)
    pieces = [(own, 0, 4, 0), (from_x, 0, 4, XN), (from_y, 0, 4, YN), (diag_lo, 0, 2, XN ^ YN), (diag_hi, 2, 2, XN ^ YN)]
    return pieces + [(permute(arr, CORE), lo, n, mask ^ CORE) for arr, lo, n, mask in pieces]


def spread_mlp(mine, other):
    same = [(mine, 0), (permute(mine, YN), YN)]
    from_x = permute(other, XN)
    cross = [(from_x, XN), (permute(from_x, YN), XN ^ YN)]
    same = same + [(permute(arr, CORE), mask ^ CORE) for arr, mask in same]
    cross = cross + [(permute(arr, CORE), mask ^ CORE) for arr, mask in cross]
    return same, cross


def qkv_kernel(plan, layer, me_ref, x_ref, vec_ref, bias_ref, cos_ref, sin_ref, *refs):
    n = len(plan)
    pieces = refs[:n]
    q_ref, k_ref, v_ref, wbuf, qkv_t, sem = refs[n:]
    me = me_ref[0]
    copies = []
    for (lo, blocks, mask), piece in zip(plan, pieces):
        origin = jnp.bitwise_xor(me, mask)
        rows = pl.ds(pl.multiple_of(origin * 128, 128), 128)
        for b in range(lo, min(lo + blocks, 3)):
            copies.append(pltpu.make_async_copy(piece.at[pl.ds((b - lo) * 128, 128)], wbuf.at[b, rows], sem.at[len(copies)]))
    for copy in copies:
        copy.start()
    normed = layer_norm_rows(x_ref[...], vec_ref[layer : layer + 1, :], vec_ref[2 + layer : 3 + layer, :])
    for copy in copies:
        copy.wait()

    def project(step, carry):
        block, chunk = step // 4, step % 4
        cols = pl.ds(pl.multiple_of(chunk * 256, 256), 256)
        out_cols = pl.ds(pl.multiple_of(step * 256, 256), 256)
        part = jnp.dot(normed, wbuf[block, :, cols], preferred_element_type=jnp.float32) + bias_ref[:, out_cols]
        qkv_t[pl.ds(pl.multiple_of(step * 256, 256), 256), :] = part.astype(jnp.bfloat16).astype(jnp.float32).T
        return carry

    lax.fori_loop(0, 12, project, 0)
    cos_t, sin_t = cos_ref[...], sin_ref[...]

    def split_head(head, carry):
        base = pl.multiple_of(head * 192, 64)
        dst = pl.multiple_of(head * 64, 64)
        for part, ref in enumerate((q_ref, k_ref, v_ref)):
            src = base + 64 * part
            if part < 2:
                lo = qkv_t[pl.ds(src, 8), :]
                hi = qkv_t[pl.ds(src + 8, 8), :]
                mixed = jnp.concatenate([lo * cos_t - hi * sin_t, hi * cos_t + lo * sin_t], axis=0)
                ref[pl.ds(dst, 16), :] = mixed.astype(jnp.bfloat16)
                ref[pl.ds(dst + 16, 48), :] = qkv_t[pl.ds(src + 16, 48), :].astype(jnp.bfloat16)
            else:
                ref[pl.ds(dst, 64), :] = qkv_t[pl.ds(src, 64), :].astype(jnp.bfloat16)
        return carry

    lax.fori_loop(0, HEADS, split_head, 0)


def qkv_project(layer, me, x, vecs, bias, cos_t, sin_t, pieces):
    plan = tuple((lo, n, mask) for _, lo, n, mask in pieces if lo < 3)
    arrays = [arr for arr, lo, _, _ in pieces if lo < 3]
    shape = jax.ShapeDtypeStruct((D, BL), jnp.bfloat16)
    return pl.pallas_call(
        functools.partial(qkv_kernel, plan, layer),
        out_shape=(shape, shape, shape),
        in_specs=[SM] + [VM] * 5 + [ANY] * len(arrays), out_specs=(VM, VM, VM),
        scratch_shapes=[
            pltpu.VMEM((3, D, D), jnp.bfloat16),
            pltpu.VMEM((3 * D, BL), jnp.float32),
            pltpu.SemaphoreType.DMA((32,)),
        ],
        compiler_params=params(24 * 2**20),
        cost_estimate=cost(2 * BL * D * 3 * D, 8 * 2**20),
        name=f"qkv{layer}",
    )(me, x, vecs, bias, cos_t, sin_t, *arrays)


NBUF = 8
AHEAD = 4


def attn_kernel(plan, layer, aliased, me_ref, x_ref, pos_ref, vec_ref, q_in, k_in, v_in, kc, vc, *refs):
    n = len(plan)
    pieces = refs[:n]
    if aliased:
        refs = refs[2:]
    ko, vo, res_ref, buf, qf, newf, scores, ctx, wbuf, in_sem, out_sem, w_sem = refs[n:]
    me = me_ref[0]
    wcopies = []
    for (lo, blocks, mask), piece in zip(plan, pieces):
        origin = jnp.bitwise_xor(me, mask)
        rows = pl.ds(pl.multiple_of(origin * 128, 128), 128)
        wcopies.append(pltpu.make_async_copy(piece.at[pl.ds((3 - lo) * 128, 128)], wbuf.at[rows], w_sem.at[len(wcopies)]))

    def fetch(src, slot, step):
        b = lax.rem(step, NBUF)
        return pltpu.make_async_copy(src.at[layer, slot], buf.at[b], in_sem.at[b])

    def flush(dst, slot, step):
        b = lax.rem(step, NBUF)
        return pltpu.make_async_copy(buf.at[b], dst.at[layer, slot], out_sem.at[b])

    for t in range(AHEAD):
        fetch(kc, t, t).start()
    for copy in wcopies:
        copy.start()
    qf[...] = q_in[...].astype(jnp.float32)
    newf[...] = k_in[...].astype(jnp.float32)
    pos = pos_ref[...]

    def k_step(slot, carry):
        fetch(kc, slot, slot).wait()

        @pl.when(slot >= NBUF - AHEAD)
        def _():
            flush(ko, slot - (NBUF - AHEAD), slot + AHEAD).wait()

        @pl.when(slot + AHEAD < SLOTS)
        def _():
            fetch(kc, slot + AHEAD, slot + AHEAD).start()

        @pl.when(slot + AHEAD >= SLOTS)
        def _():
            fetch(vc, slot + AHEAD - SLOTS, slot + AHEAD).start()

        b = lax.rem(slot, NBUF)
        hit = pos == slot
        for head in range(HEADS):
            rows = pl.ds(head * HEAD, HEAD)
            key = jnp.where(hit, newf[rows, :], buf[b, rows, :].astype(jnp.float32))
            buf[b, rows, :] = key.astype(jnp.bfloat16)
            scores[slot, pl.ds(head, 1), :] = jnp.sum(key * qf[rows, :], axis=0, keepdims=True)
        flush(ko, slot, slot).start()
        return carry

    lax.fori_loop(0, SLOTS, k_step, 0)

    slot_ids = lax.broadcasted_iota(jnp.int32, (SLOTS, 1, 1), 0)
    keep = slot_ids <= pos[None]
    for head in range(0, HEADS, 8):
        part = scores[:, pl.ds(head, 8), :] * (HEAD ** -0.5)
        part = jnp.where(keep, part, -jnp.inf)
        top = jnp.max(part, axis=0, keepdims=True)
        expd = jnp.exp(part - top)
        probs = expd / jnp.sum(expd, axis=0, keepdims=True)
        scores[:, pl.ds(head, 8), :] = probs.astype(jnp.bfloat16).astype(jnp.float32)
    newf[...] = v_in[...].astype(jnp.float32)
    ctx[...] = jnp.zeros_like(ctx)

    def v_step(slot, carry):
        step = slot + SLOTS
        fetch(vc, slot, step).wait()

        @pl.when(slot < NBUF - AHEAD)
        def _():
            flush(ko, slot + SLOTS - (NBUF - AHEAD), step + AHEAD).wait()

        @pl.when(slot >= NBUF - AHEAD)
        def _():
            flush(vo, slot - (NBUF - AHEAD), step + AHEAD).wait()

        @pl.when(slot + AHEAD < SLOTS)
        def _():
            fetch(vc, slot + AHEAD, step + AHEAD).start()

        b = lax.rem(step, NBUF)
        hit = pos == slot
        for head in range(HEADS):
            rows = pl.ds(head * HEAD, HEAD)
            val = jnp.where(hit, newf[rows, :], buf[b, rows, :].astype(jnp.float32))
            buf[b, rows, :] = val.astype(jnp.bfloat16)
            ctx[rows, :] += scores[slot, pl.ds(head, 1), :] * val
        flush(vo, slot, step).start()
        return carry

    lax.fori_loop(0, SLOTS, v_step, 0)
    for t in range(SLOTS - (NBUF - AHEAD), SLOTS):
        flush(vo, t, t + SLOTS).wait()

    for copy in wcopies:
        copy.wait()
    ctx_rows = ctx[...].T.astype(jnp.bfloat16)
    bias = vec_ref[8 + layer : 9 + layer, :] + vec_ref[10 + layer : 11 + layer, :]
    for c in range(4):
        cols = pl.ds(c * 256, 256)
        proj = jnp.dot(ctx_rows, wbuf[:, cols], preferred_element_type=jnp.float32)
        res_ref[:, cols] = x_ref[:, cols].astype(jnp.float32) + proj + bias[:, c * 256 : (c + 1) * 256]


def attend(layer, me, x, pos, vecs, q_t, k_t, v_t, kc, vc, pieces, prev):
    used = [(arr, lo, n, mask) for arr, lo, n, mask in pieces if lo + n == 4]
    plan = tuple((lo, n, mask) for _, lo, n, mask in used)
    arrays = [arr for arr, _, _, _ in used]
    cache = jax.ShapeDtypeStruct(kc.shape, kc.dtype)
    args = [me, x, pos, vecs, q_t, k_t, v_t, kc, vc, *arrays]
    aliases = {}
    if prev is not None:
        aliases = {len(args): 0, len(args) + 1: 1}
        args += list(prev)
    return pl.pallas_call(
        functools.partial(attn_kernel, plan, layer, prev is not None),
        out_shape=(cache, cache, jax.ShapeDtypeStruct((BL, D), jnp.float32)),
        in_specs=[SM] + [VM] * 6 + [ANY] * (len(args) - 7), out_specs=(ANY, ANY, VM),
        scratch_shapes=[
            pltpu.VMEM((NBUF, D, BL), jnp.bfloat16),
            pltpu.VMEM((D, BL), jnp.float32),
            pltpu.VMEM((D, BL), jnp.float32),
            pltpu.VMEM((SLOTS, HEADS, BL), jnp.float32),
            pltpu.VMEM((D, BL), jnp.float32),
            pltpu.VMEM((D, D), jnp.bfloat16),
            pltpu.SemaphoreType.DMA((NBUF,)),
            pltpu.SemaphoreType.DMA((NBUF,)),
            pltpu.SemaphoreType.DMA((8,)),
        ],
        input_output_aliases=aliases,
        compiler_params=params(24 * 2**20),
        cost_estimate=cost(25 * 10**8, 67 * 10**6),
        name=f"attend{layer}",
    )(*args)


def mlp_kernel(same_plan, cross_plan, layer, me_ref, mine_ref, theirs_ref, vec_ref, bias_ref, *refs):
    n = len(same_plan)
    m = len(cross_plan)
    same, cross = refs[:n], refs[n : n + m]
    out_mine, out_theirs, win, wdn, h_ref, act_ref, sem = refs[n + m :]
    me = me_ref[0]
    in_copies, down_copies = [], []
    for mask, piece in list(zip(same_plan, same)) + list(zip(cross_plan, cross)):
        origin = jnp.bitwise_xor(me, mask)
        rows = pl.ds(pl.multiple_of(origin * 128, 128), 128)
        for yy in range(2):
            in_copies.append(pltpu.make_async_copy(piece.at[pl.ds(128 * yy, 128)], win.at[yy, rows], sem.at[len(in_copies)]))
    for mask, piece in zip(same_plan, same):
        origin = jnp.bitwise_xor(me, mask)
        start = pl.multiple_of((origin // 4) * 1024 + (origin % 2) * 512, 512)
        down_copies.append(pltpu.make_async_copy(piece.at[pl.ds(256, 512)], wdn.at[pl.ds(start, 512)], sem.at[16 + len(down_copies)]))
    for copy in in_copies + down_copies:
        copy.start()
    gain, bias = vec_ref[4 + layer : 5 + layer, :], vec_ref[6 + layer : 7 + layer, :]
    h_ref[pl.ds(0, BL), :] = layer_norm_rows(theirs_ref[...], gain, bias)
    h_ref[pl.ds(BL, BL), :] = layer_norm_rows(mine_ref[...], gain, bias)
    for copy in in_copies:
        copy.wait()

    def widen(step, carry):
        block, chunk = step // 4, step % 4
        cols = pl.ds(pl.multiple_of(chunk * 256, 256), 256)
        out_cols = pl.ds(pl.multiple_of(step * 256, 256), 256)
        pre = jnp.dot(h_ref[...], win[block, :, cols], preferred_element_type=jnp.float32) + bias_ref[:, out_cols]
        act_ref[:, out_cols] = (0.5 * pre * (1.0 + lax.erf(pre * (0.5 ** 0.5)))).astype(jnp.bfloat16)
        return carry

    lax.fori_loop(0, 8, widen, 0)
    for copy in down_copies:
        copy.wait()

    def narrow(step, carry):
        cols = pl.ds(pl.multiple_of(step * 256, 256), 256)
        part = jnp.dot(act_ref[...], wdn[:, cols], preferred_element_type=jnp.float32)
        out_theirs[:, cols] = part[:BL]
        out_mine[:, cols] = part[BL:]
        return carry

    lax.fori_loop(0, 4, narrow, 0)


def mlp(layer, me, mine, theirs, vecs, bias, same, cross):
    shape = jax.ShapeDtypeStruct((BL, D), jnp.float32)
    return pl.pallas_call(
        functools.partial(mlp_kernel, tuple(m for _, m in same), tuple(m for _, m in cross), layer),
        out_shape=(shape, shape),
        in_specs=[SM] + [VM] * 4 + [ANY] * (len(same) + len(cross)), out_specs=(VM, VM),
        scratch_shapes=[
            pltpu.VMEM((2, D, D), jnp.bfloat16),
            pltpu.VMEM((2 * D, D), jnp.bfloat16),
            pltpu.VMEM((2 * BL, D), jnp.bfloat16),
            pltpu.VMEM((2 * BL, 2 * D), jnp.bfloat16),
            pltpu.SemaphoreType.DMA((20,)),
        ],
        compiler_params=params(32 * 2**20),
        cost_estimate=cost(2 * 2 * BL * D * 4 * D, 14 * 2**20),
        name=f"mlp{layer}",
    )(me, mine, theirs, vecs, bias, *[a for a, _ in same], *[a for a, _ in cross])


def final_kernel(res_ref, mine_ref, theirs_ref, vec_ref, out_ref):
    hidden = (res_ref[...] + (mine_ref[...] + theirs_ref[...])).astype(jnp.bfloat16)
    out_ref[...] = layer_norm_rows(hidden, vec_ref[12:13, :], vec_ref[13:14, :])


def merge_kernel(res_ref, mine_ref, theirs_ref, out_ref):
    out_ref[...] = (res_ref[...] + (mine_ref[...] + theirs_ref[...])).astype(jnp.bfloat16)


def small_call(kernel, name, *args):
    return pl.pallas_call(
        kernel, out_shape=jax.ShapeDtypeStruct((BL, D), jnp.bfloat16),
        in_specs=[VM] * len(args), out_specs=VM, name=name,
        compiler_params=params(16 * 2**20), cost_estimate=cost(10**7, 4 * 2**20),
    )(*args)


def solution(mesh):
    row_spec = P('dp', None)
    vec_spec = P(None, 'dp')
    mat_spec = P(None, 'dp', None)
    cache_spec = P(None, 'dp', None, None, None)
    in_specs = (row_spec, P('dp'), cache_spec, cache_spec, vec_spec, vec_spec, vec_spec, vec_spec, mat_spec, vec_spec, mat_spec, vec_spec, mat_spec, vec_spec, mat_spec, vec_spec, P('dp'), P('dp'))
    out_specs = (row_spec, cache_spec, cache_spec)

    def device_step(x_embed, positions, k_cache, v_cache, ln1_gain, ln1_bias, ln2_gain, ln2_bias, w_qkv, b_qkv, w_out, b_out, w_in, b_in, w_down, b_down, lnf_gain, lnf_bias):
        index = lax.axis_index('dp').astype(jnp.int32)
        xb = (index // 2) % 2
        me = index.reshape(1)
        half = xb.reshape(1)

        to_minor = lambda c: jnp.transpose(c, (0, 2, 3, 4, 1)).reshape(2, SLOTS, D, BL)
        kc, vc = to_minor(k_cache), to_minor(v_cache)

        attn_pieces = [spread_attn(pack_attn(l, w_qkv, w_out)) for l in range(2)]
        mlp_pieces = [spread_mlp(*pack_mlp(l, half, w_in, w_down)) for l in range(2)]

        rows = [ln1_gain, ln1_bias, ln2_gain, ln2_bias, b_out, b_down, lnf_gain, lnf_bias, b_qkv, b_in]
        small = jnp.concatenate([r.reshape(-1) for r in rows]).reshape(28, 128)
        small = lax.all_gather(small, 'dp', axis=0, tiled=False).astype(jnp.float32)
        vecs = small[:, :14].transpose(1, 0, 2).reshape(14, D)
        b_qkv_rows = [small[:, 14 + 3 * l : 17 + 3 * l].reshape(1, 3 * D) for l in range(2)]
        b_in_rows = []
        for l in range(2):
            blocks = small[:, 20 + 4 * l : 24 + 4 * l].reshape(2, 2, D)
            b_in_rows.append(lax.dynamic_index_in_dim(blocks, xb, axis=1, keepdims=False).reshape(1, 2 * D))

        inv_freq = 1.0 / (ROPE_BASE ** (jnp.arange(0, 16, 2).astype(jnp.float32) / 16))
        angles = inv_freq[:, None] * positions.astype(jnp.float32)[None, :]
        cos_t, sin_t = jnp.cos(angles), jnp.sin(angles)
        pos = positions.reshape(1, BL)

        hidden = x_embed
        caches = None
        out = None
        for l in range(2):
            theirs = permute(hidden, XN)
            q_t, k_t, v_t = qkv_project(l, me, hidden, vecs, b_qkv_rows[l], cos_t, sin_t, attn_pieces[l])
            m_mine, m_theirs = mlp(l, me, hidden, theirs, vecs, b_in_rows[l], *mlp_pieces[l])
            got = permute(m_theirs, XN)
            ko, vo, res = attend(l, me, hidden, pos, vecs, q_t, k_t, v_t, kc, vc, attn_pieces[l], caches)
            caches = (ko, vo)
            if l == 0:
                hidden = small_call(merge_kernel, "merge0", res, m_mine, got)
            else:
                out = small_call(final_kernel, "final", res, m_mine, got, vecs)
        back = lambda c: jnp.transpose(c.reshape(2, SLOTS, HEADS, HEAD, BL), (0, 4, 1, 2, 3))
        return out, back(caches[0]), back(caches[1])

    return jax.shard_map(device_step, mesh=mesh, in_specs=in_specs, out_specs=out_specs, check_vma=False)
```
